256 devices in a mesh: seq: 64 (over z, y, core), head: 4 (over x).
Axes of the slice: x: 4, y: 4, z: 8, core: 2. Of those that a mesh axis runs over, the one named last changes fastest.
Arguments:
- query_rows: bfloat16 [131072, 4096], P(('seq', 'head')), may hold values from -200 to 200
- key_rows: bfloat16 [131072, 512], P(('seq', 'head')), may hold values from -18 to 18
- value_rows: bfloat16 [131072, 512], P(('seq', 'head')), may hold values from -6 to 6
- random_table: int32 [1024, 4, 3], replicated, may hold values from 0 to 1023, as said below
- global_blocks: int32 [2], replicated, may hold values from 0 to 1023
Outputs:
- attended: bfloat16 [131072, 4096], P(('seq', 'head'))
The draws below stay inside these ranges and needn't reach their ends.
Inputs may be any that keep to these rules, and one draw needn't show every extreme that they name: `random_table`: for each of the 4 head groups and each aligned run of 16 query blocks (those of one index of seq), with the owner of block j being j // 16: at most 2 of the run's 3 * 16 entries name blocks of one owner, and they name at most 1 distinct blocks of one owner; both bounds are reached.
All inputs are finite; a program needn't handle non-finite values.
Results may differ from the reference program's by a relative error of at most 0.0029.
Values may be sent and summed in bfloat16 or wider, within the bound.
A program may use at most 128 MiB of HBM per device.

```python
import math
import jax
import jax.numpy as jnp
from jax import lax

BLOCK = 128
HEAD_DIM = 128
Q_HEADS = 32
KV_HEADS = 4
GLOBALS = 2
RANDOM = 3
BLK_DEV = 16
BLOCKS = 1024
TOKENS = 131072
CAP_RAW = 2
DISTINCT = 1


def pair_rows(key):
    normal_keys = jax.random.normal(jax.random.fold_in(key, 701), (TOKENS, KV_HEADS * HEAD_DIM), jnp.float32)
    key_part = jnp.clip(3.0 * normal_keys, -18.0, 18.0)
    queries = jnp.clip(jax.random.normal(jax.random.fold_in(key, 702), (TOKENS, Q_HEADS * HEAD_DIM), jnp.float32), -6.0, 6.0)
    return (queries, key_part)


def draw_query_rows(key, part):
    return pair_rows(key)[0].astype(jnp.bfloat16)


def draw_key_rows(key, part):
    return pair_rows(key)[1].astype(jnp.bfloat16)


def draw_random_table(key, part):
    entry_count = RANDOM * BLK_DEV
    seq_count = BLOCKS // BLK_DEV
    group_count = (entry_count + CAP_RAW - 1) // CAP_RAW

    def one_run(run_key):
        owners = jax.random.permutation(jax.random.fold_in(run_key, 1), seq_count)
        groups = jnp.arange(entry_count, dtype=jnp.int32) // CAP_RAW
        pair_index = jnp.arange(entry_count, dtype=jnp.int32) % CAP_RAW // 2
        group_keys = jax.vmap(lambda which: jax.random.fold_in(run_key, 50 + which))(jnp.arange(group_count, dtype=jnp.int32))
        picks = jax.vmap(lambda gkey: jax.random.permutation(gkey, BLK_DEV)[:DISTINCT])(group_keys)
        local_ids = picks[groups, pair_index]
        references = owners[groups] * BLK_DEV + local_ids
        shuffle = jax.random.permutation(jax.random.fold_in(run_key, 5), entry_count)
        return references[shuffle].reshape(BLK_DEV, RANDOM)
    run_keys = jax.vmap(lambda which: jax.random.fold_in(key, 900 + which))(jnp.arange(seq_count * KV_HEADS, dtype=jnp.int32))
    tables = jax.vmap(one_run)(run_keys).reshape(seq_count, KV_HEADS, BLK_DEV, RANDOM)
    return tables.transpose(0, 2, 1, 3).reshape(BLOCKS, KV_HEADS, RANDOM).astype(jnp.int32)


def level_of(own_key, extent, pieces, low, top_value):
    factor_of = 1.0
    for position, shards_of in pieces:
        heights = jax.random.uniform(jax.random.fold_in(jax.random.fold_in(own_key, 6), position), (shards_of,), jnp.float32, low / len(pieces), top_value / len(pieces))
        factor_of = factor_of * jnp.repeat(jnp.exp(heights), extent[position] // shards_of).reshape((-1,) + (1,) * (len(extent) - 1 - position))
    return factor_of


def noise(stream_key, shape, deviation, most, shards=(), kind=jnp.bfloat16):
    drawn = deviation * jax.random.normal(stream_key, shape, jnp.float32)
    if shards:
        drawn = drawn * level_of(stream_key, shape, shards, -0.22, 0.18)
    return jnp.clip(drawn, -most, most).astype(kind)


def setup_inputs(seed: int = 0) -> dict:
    arg_keys = jax.random.split(jax.random.key(seed), 6)
    return {
        "query_rows": draw_query_rows(jax.random.fold_in(arg_keys[5], 71), 0),
        "key_rows": draw_key_rows(jax.random.fold_in(arg_keys[5], 71), 0),
        "value_rows": noise(arg_keys[2], (TOKENS, KV_HEADS * HEAD_DIM), 1.0, 6.0, ((0, 256),)),
        "random_table": draw_random_table(jax.random.fold_in(arg_keys[5], 71), 0),
        "global_blocks": jax.random.randint(arg_keys[4], (GLOBALS,), 0, BLOCKS).astype(jnp.int32),
    }


def reference(query_rows, key_rows, value_rows, random_table, global_blocks):
    grouping = Q_HEADS // KV_HEADS
    score_scale = 1.0 / math.sqrt(HEAD_DIM)
    query_split = query_rows.reshape(BLOCKS, BLOCK, KV_HEADS, grouping, HEAD_DIM)
    key_heads = key_rows.reshape(BLOCKS, BLOCK, KV_HEADS, HEAD_DIM).transpose(2, 0, 1, 3)
    value_heads = value_rows.reshape(BLOCKS, BLOCK, KV_HEADS, HEAD_DIM).transpose(2, 0, 1, 3)
    head_range = jnp.arange(KV_HEADS, dtype=jnp.int32)[:, None]

    def one_block(block_index):
        before = jnp.maximum(block_index - 1, 0)
        following = jnp.minimum(block_index + 1, BLOCKS - 1)
        window = jnp.stack([before, block_index, following]).astype(jnp.int32)
        shared = jnp.concatenate([window, global_blocks.astype(jnp.int32)])
        chosen = jnp.concatenate([jnp.broadcast_to(shared, (KV_HEADS, shared.shape[0])), random_table[block_index].astype(jnp.int32)], axis=1)
        key_sel = key_heads[head_range, chosen].reshape(KV_HEADS, -1, HEAD_DIM)
        value_sel = value_heads[head_range, chosen].reshape(KV_HEADS, -1, HEAD_DIM)
        block_flags = jnp.concatenate([jnp.stack([block_index > 0, block_index >= 0, block_index < BLOCKS - 1]), jnp.ones((GLOBALS + RANDOM,), dtype=bool)])
        usable = jnp.repeat(block_flags, BLOCK)
        scores = jnp.einsum('tkgd,ksd->kgts', query_split[block_index].astype(jnp.float32), key_sel.astype(jnp.float32)) * score_scale
        scores = jnp.where(usable, scores, -1e+30)
        row_max = lax.optimization_barrier(jnp.max(scores, axis=-1, keepdims=True))
        weights = jnp.exp(scores - row_max)
        row_total = lax.optimization_barrier(jnp.sum(weights, axis=-1))
        rounded = weights.astype(jnp.bfloat16)
        mixed = jnp.einsum('kgts,ksd->tkgd', rounded.astype(jnp.float32), value_sel.astype(jnp.float32))
        mixed = mixed / jnp.transpose(row_total, (2, 0, 1))[..., None]
        return mixed.reshape(BLOCK, Q_HEADS * HEAD_DIM).astype(jnp.bfloat16)
    result = lax.map(one_block, jnp.arange(BLOCKS, dtype=jnp.int32))
    return result.reshape(TOKENS, Q_HEADS * HEAD_DIM)
```

```python
import math

import jax
import jax.numpy as jnp
from jax import lax
from jax.experimental import pallas as pl
from jax.experimental.pallas import tpu as pltpu
from jax.sharding import PartitionSpec as P

BLOCK = 128
DIM = 128
GLOBALS = 2
RANDOM = 3
GROUP = 8
SCALE = 1.0 / math.sqrt(DIM)
NT = (((1,), (1,)), ((), ()))


def stacked(q_tile):
    return jnp.concatenate([q_tile[:, j * DIM : (j + 1) * DIM] for j in range(GROUP)], axis=0)


def near_kernel(edge, q, k0, k1, k2, v0, v1, v2, kg, vg, acc, stat):
    i = pl.program_id(0)
    rows = stacked(q[...])
    dot = lambda k: lax.dot_general(rows, k[...], NT, preferred_element_type=jnp.float32) * SCALE
    no_prev = jnp.logical_and(edge[0] == 1, i == 0)
    no_next = jnp.logical_and(edge[1] == 1, i == pl.num_programs(0) - 1)
    s0 = jnp.where(no_prev, -1e30, dot(k0))
    s2 = jnp.where(no_next, -1e30, dot(k2))
    scores = jnp.concatenate([s0, dot(k1), s2, dot(kg)], axis=1)
    top = jnp.max(scores, axis=1, keepdims=True)
    weights = jnp.exp(scores - top)
    total = jnp.sum(weights, axis=1, keepdims=True)
    values = jnp.concatenate([v0[...], v1[...], v2[...], vg[...]], axis=0)
    acc[...] = jnp.dot(weights.astype(jnp.bfloat16), values, preferred_element_type=jnp.float32)
    lane = lax.broadcasted_iota(jnp.int32, stat.shape, 1)
    stat[...] = jnp.where(lane < 64, top, total)


def far_kernel(q, kr, vr, acc, stat, out):
    rows = stacked(q[...])
    keys = kr[0].reshape(RANDOM * BLOCK, DIM)
    values = vr[0].reshape(RANDOM * BLOCK, DIM)
    scores = lax.dot_general(rows, keys, NT, preferred_element_type=jnp.float32) * SCALE
    top = stat[:, 0:1]
    total = stat[:, 64:65]
    peak = jnp.maximum(jnp.max(scores, axis=1, keepdims=True), top)
    weights = jnp.exp(scores - peak)
    shrink = jnp.exp(top - peak)
    total = total * shrink + jnp.sum(weights, axis=1, keepdims=True)
    mixed = acc[...] * shrink + jnp.dot(
        weights.astype(jnp.bfloat16), values, preferred_element_type=jnp.float32
    )
    mixed = (mixed / total).astype(jnp.bfloat16)
    for j in range(GROUP):
        out[:, j * DIM : (j + 1) * DIM] = mixed[j * BLOCK : (j + 1) * BLOCK]


def on_device(query_rows, key_rows, value_rows, random_table, global_blocks):
    rows, width = query_rows.shape
    seq_count = lax.axis_size("seq")
    heads = lax.axis_size("head")
    seq_index = lax.axis_index("seq")
    head_index = lax.axis_index("head")
    here = rows // BLOCK
    run = here * heads
    linear = seq_index * heads + head_index
    devices = seq_count * heads

    split = lambda part: lax.all_to_all(part, "head", split_axis=1, concat_axis=0, tiled=True)
    run_keys = split(key_rows).reshape(run, BLOCK, DIM)
    run_values = split(value_rows).reshape(run, BLOCK, DIM)

    table_head = lax.dynamic_index_in_dim(random_table, head_index, 1, keepdims=False)
    refs = table_head.reshape(seq_count, run * RANDOM)
    sources = jnp.max(jnp.where(refs // run == seq_index, refs % run, 0), axis=1)
    mine = lax.dynamic_index_in_dim(refs, seq_index, 0, keepdims=False)
    owners = mine // run

    def fetch(blocks):
        sent = jnp.take(blocks, sources, axis=0)
        got = lax.all_to_all(sent, "seq", split_axis=0, concat_axis=0, tiled=True)
        named = jnp.take(got, owners, axis=0).reshape(heads, here * RANDOM, BLOCK, DIM)
        return lax.all_to_all(named, "head", split_axis=0, concat_axis=0, tiled=True)

    far_keys = fetch(run_keys)
    far_values = fetch(run_values)

    paired = jnp.concatenate([key_rows, value_rows], axis=1)
    axes = ("seq", "head")
    before = lax.ppermute(paired[rows - BLOCK :], axes, [(n, n + 1) for n in range(devices - 1)])
    after = lax.ppermute(paired[:BLOCK], axes, [(n + 1, n) for n in range(devices - 1)])
    local = paired.reshape(here, BLOCK, paired.shape[1])
    owned = jnp.take(local, global_blocks % here, axis=0)
    owned = jnp.where((global_blocks // here == linear)[:, None, None], owned, jnp.zeros_like(owned))
    shared = lax.psum(owned, axes).reshape(GLOBALS * BLOCK, paired.shape[1])
    wide = jnp.concatenate([before, paired, after], axis=0)

    tasks = here * heads
    lines = GROUP * BLOCK
    tile = lambda fn: pl.BlockSpec((BLOCK, DIM), fn)
    q_spec = pl.BlockSpec((BLOCK, GROUP * DIM), lambda i, h: (i, h))
    state_spec = pl.BlockSpec((lines, DIM), lambda i, h: (i * heads + h, 0))
    state = jax.ShapeDtypeStruct((tasks * lines, DIM), jnp.float32)
    edge = jnp.stack([linear == 0, linear == devices - 1]).astype(jnp.int32)
    acc, stat = pl.pallas_call(
        near_kernel,
        grid=(here, heads),
        out_shape=(state, state),
        in_specs=[pl.BlockSpec(memory_space=pltpu.SMEM), q_spec]
        + [tile(lambda i, h, o=o: (i + o, h)) for o in range(3)]
        + [tile(lambda i, h, o=o: (i + o, heads + h)) for o in range(3)]
        + [
            pl.BlockSpec((GLOBALS * BLOCK, DIM), lambda i, h: (0, h)),
            pl.BlockSpec((GLOBALS * BLOCK, DIM), lambda i, h: (0, heads + h)),
        ],
        out_specs=(state_spec, state_spec),
        cost_estimate=pl.CostEstimate(flops=6_000_000_000, bytes_accessed=24_000_000, transcendentals=0),
        name="near",
    )(edge, query_rows, wide, wide, wide, wide, wide, wide, shared, shared)
    far_spec = pl.BlockSpec((1, RANDOM, BLOCK, DIM), lambda i, h: (h, i, 0, 0))
    return pl.pallas_call(
        far_kernel,
        grid=(here, heads),
        out_shape=jax.ShapeDtypeStruct((rows, width), jnp.bfloat16),
        in_specs=[q_spec, far_spec, far_spec, state_spec, state_spec],
        out_specs=q_spec,
        cost_estimate=pl.CostEstimate(flops=4_000_000_000, bytes_accessed=24_000_000, transcendentals=0),
        name="far",
    )(query_rows, far_keys, far_values, acc, stat)


def solution(mesh):
    split = P(("seq", "head"), None)
    return jax.shard_map(
        on_device,
        mesh=mesh,
        in_specs=(split, split, split, P(), P()),
        out_specs=split,
        check_vma=False,
    )
```

```python
import math

import jax
import jax.numpy as jnp
from jax import lax
from jax.experimental import pallas as pl
from jax.experimental.pallas import tpu as pltpu
from jax.sharding import PartitionSpec as P

BLOCK = 128
DIM = 128
GLOBALS = 2
RANDOM = 3
GROUP = 8
HALF = 4
SCALE = 1.0 / math.sqrt(DIM)
NT = (((1,), (1,)), ((), ()))
MESH = pl.DeviceIdType.MESH

ZS, YS, CS, XS = 8, 4, 2, 4
PLANE = YS * CS
HERE = 4
RUN = HERE * XS
NAMED = HERE * RANDOM
TASKS = HERE * XS
LINES = GROUP * BLOCK
PIECE = BLOCK // PLANE

CHUNKS = ((0, 0, 64), (0, 64, 64), (1, 0, 64), (1, 64, 32), (1, 96, 32))
COUNT = len(CHUNKS)
KEYS = (0, 1)
VALUES = (2, 3, 4)
SPOT = {0: 0, 1: 1, 7: 2, 2: 3, 6: 4, 3: 5, 5: 6, 4: 7}


def body(
    table, q_hbm, k_hbm, v_hbm, out_hbm,
    ring, outbox, inbox, named, given, probs, qbuf, kwin, vwin, acc, stat,
    gpart, gfrom, gring, gmine, gall,
    x1s, x1r, zs, zr, ys, yr, x2s, x2r, hs, hr,
    gbs, gbr, gcs, gcr, gds, gdr, ghs, ghr, local, outs,
):
    seq = lax.axis_index("seq")
    x = lax.axis_index("head")
    z, yc = seq // PLANE, seq % PLANE
    y, c = yc // CS, yc % CS
    linear = seq * XS + x
    total = ZS * PLANE * XS

    def in_plane(p):
        return lax.rem(y + p // CS, YS) * CS + lax.rem(c + p % CS, CS)

    def at_x(t):
        return lax.rem(x + t, XS)

    above = lax.rem(z + 1, ZS) * PLANE + yc
    below = lax.rem(z + ZS - 1, ZS) * PLANE + yc
    ahead = lax.rem(linear + 1, total)
    behind = lax.rem(linear + total - 1, total)
    ahead = (ahead // XS, lax.rem(ahead, XS))
    behind = (behind // XS, lax.rem(behind, XS))

    def remote(src, dst, send, recv, where):
        return pltpu.make_async_remote_copy(
            src_ref=src, dst_ref=dst, send_sem=send, recv_sem=recv,
            device_id=where, device_id_type=MESH,
        )

    def own_part(j):
        kind, first, size = CHUNKS[j]
        source = (k_hbm, v_hbm)[kind]
        columns = pl.ds(pl.multiple_of(x * DIM, DIM), DIM)
        return pltpu.make_async_copy(
            source.at[:, first : first + size, columns],
            ring[j][0].at[pl.ds(x * HERE, HERE)],
            local.at[j],
        )

    keep_k = pltpu.make_async_copy(k_hbm, kwin.at[1 : 1 + HERE], local.at[COUNT])
    keep_v = pltpu.make_async_copy(v_hbm, vwin.at[1 : 1 + HERE], local.at[COUNT + 1])
    keep_q = pltpu.make_async_copy(q_hbm, qbuf, local.at[COUNT + 2])

    barrier = pltpu.get_barrier_semaphore()
    partners = [(seq, at_x(t)) for t in range(1, XS)]
    partners += [(z * PLANE + in_plane(p), x) for p in range(1, PLANE)]
    partners += [(above, x), (below, x), ahead, behind]
    for partner in partners:
        pl.semaphore_signal(barrier, inc=1, device_id=partner, device_id_type=MESH)
    for j in range(COUNT):
        own_part(j).start()
    keep_k.start()
    keep_v.start()
    keep_q.start()
    pl.semaphore_wait(barrier, len(partners))

    def to_head(j, t):
        kind, first, size = CHUNKS[j]
        source = (k_hbm, v_hbm)[kind]
        columns = pl.ds(pl.multiple_of(at_x(t) * DIM, DIM), DIM)
        return remote(
            source.at[:, first : first + size, columns],
            ring[j][0].at[pl.ds(x * HERE, HERE)],
            x1s.at[j, t - 1], x1r.at[j, t - 1], (seq, at_x(t)),
        )

    for j in range(COUNT):
        for t in range(1, XS):
            to_head(j, t).start()
    sides = [
        remote(k_hbm.at[HERE - 1], kwin.at[0], hs.at[0], hr.at[0], ahead),
        remote(v_hbm.at[HERE - 1], vwin.at[0], hs.at[1], hr.at[1], ahead),
        remote(k_hbm.at[0], kwin.at[HERE + 1], hs.at[2], hr.at[2], behind),
        remote(v_hbm.at[0], vwin.at[HERE + 1], hs.at[3], hr.at[3], behind),
    ]
    for side in sides:
        side.start()

    def hop(j, way, step):
        before, after = step - 1, step
        if way:
            before, after = (ZS - before) % ZS, ZS - after
        src, dst = ring[j][before], ring[j][after]
        if step == ZS // 2:
            cut = slice(RUN // 2, RUN) if way else slice(0, RUN // 2)
            src, dst = src.at[cut], dst.at[cut]
        return remote(
            src, dst, zs.at[j, way, step - 1], zr.at[j, way, step - 1],
            (below if way else above, x),
        )

    def choose(j, d):
        size = CHUNKS[j][2]
        for p in range(PLANE):
            block = ring[j][d][table[d * PLANE + in_plane(p)]]
            if p:
                outbox[j][p - 1, SPOT[d]] = block
            else:
                inbox[j][SPOT[d]] = block

    def post(j, low, high):
        for p in range(1, PLANE):
            remote(
                outbox[j].at[p - 1, low:high],
                inbox[j].at[p * ZS + low : p * ZS + high],
                ys.at[j], yr.at[j], (z * PLANE + in_plane(p), x),
            ).start()

    def ring_start(j):
        own_part(j).wait()
        for t in range(1, XS):
            to_head(j, t).wait_recv()
        hop(j, 0, 1).start()
        hop(j, 1, 1).start()
        choose(j, 0)

    def ring_step(j, step):
        hop(j, 0, step).wait_recv()
        hop(j, 1, step).wait_recv()
        if step < ZS // 2:
            hop(j, 0, step + 1).start()
            hop(j, 1, step + 1).start()
            choose(j, step)
            choose(j, ZS - step)
            low = 0 if step == 1 else 2 * step - 1
            post(j, low, 2 * step + 1)
        else:
            choose(j, step)
            post(j, ZS - 1, ZS)

    def give(j, t):
        return remote(
            named[j].at[t - 1], given[j].at[t], x2s.at[j, t - 1], x2r.at[j, t - 1],
            (seq, at_x(t)),
        )

    def hand_out(j):
        whole = inbox[j].at[ZS : PLANE * ZS]
        pltpu.make_async_copy(whole, whole, yr.at[j]).wait()
        for t in [1, 2, 3, 0]:
            base = PLANE * ZS + at_x(t) * NAMED

            def entry(e, carry):
                block = inbox[j][table[base + e]]
                if t:
                    named[j][t - 1, e] = block
                else:
                    given[j][0, e] = block
                return carry

            lax.fori_loop(0, NAMED, entry, 0)
            if t:
                give(j, t).start()

    def take(j):
        for t in range(1, XS):
            give(j, t).wait_recv()

    tail = PLANE * ZS + XS * NAMED

    def split_globals():
        for g in range(GLOBALS):
            block = table[tail + g]
            for j in range(COUNT):
                kind, first, size = CHUNKS[j]
                rows = ring[j][0][block]
                for a in range(size // PIECE):
                    gpart[first // PIECE + a, g, kind] = rows[a * PIECE : (a + 1) * PIECE]
        gfrom[0] = gpart[yc]
        for p in range(1, PLANE):
            there = in_plane(p)
            remote(
                gpart.at[there], gfrom.at[p], gbs, gbr, (z * PLANE + there, x)
            ).start()

    def hop_globals(n):
        if n < 4:
            return remote(gring.at[n], gring.at[n + 1], gcs.at[n], gcr.at[n], (above, x))
        before = (ZS - (n - 4)) % ZS
        return remote(
            gring.at[before], gring.at[ZS - (n - 3)], gcs.at[n], gcr.at[n], (below, x)
        )

    def ring_globals():
        whole = gfrom.at[1:PLANE]
        pltpu.make_async_copy(whole, whole, gbr).wait()
        for g in range(GLOBALS):
            gring[0, g] = gfrom[table[tail + GLOBALS + g], g]
        hop_globals(0).start()
        hop_globals(4).start()

    def pass_globals(n):
        hop_globals(n).wait_recv()
        if n not in (3, 6):
            hop_globals(n + 1).start()

    def join_globals():
        for g in range(GLOBALS):
            piece = gring[table[tail + 2 * GLOBALS + g], g]
            gmine[g] = piece
            gall[0, yc, g] = piece
        for p in range(1, PLANE):
            remote(
                gmine, gall.at[0, yc], gds, gdr, (z * PLANE + in_plane(p), x)
            ).start()

    def widen(t):
        return remote(gall.at[0], gall.at[t], ghs.at[t - 1], ghr.at[t - 1], (seq, at_x(t)))

    def spread_globals():
        whole = gfrom.at[1:PLANE]
        pltpu.make_async_copy(whole, whole, gdr).wait()
        for t in range(1, XS):
            widen(t).start()

    lane = lax.broadcasted_iota(jnp.int32, (HALF * BLOCK, DIM), 1)

    def place(n):
        i, t = n // XS, lax.rem(n, XS)
        return i, t, lax.rem(x + XS - t, XS)

    def queries(i, h, part):
        first = (h * GROUP + part * HALF) * DIM
        rows = pl.ds(pl.multiple_of(i * BLOCK, BLOCK), BLOCK)
        return jnp.concatenate(
            [
                qbuf[rows, pl.ds(pl.multiple_of(first + m * DIM, DIM), DIM)]
                for m in range(HALF)
            ],
            axis=0,
        )

    def near(n, carry):
        i, t, h = place(n)
        columns = pl.ds(pl.multiple_of(h * DIM, DIM), DIM)
        keys = kwin[pl.ds(i, 3), :, columns].reshape(3 * BLOCK, DIM)
        values = vwin[pl.ds(i, 3), :, columns].reshape(3 * BLOCK, DIM)
        no_prev = jnp.logical_and(linear == 0, i == 0)
        no_next = jnp.logical_and(linear == total - 1, i == HERE - 1)
        spot = lax.broadcasted_iota(jnp.int32, (1, 3 * BLOCK), 1)
        low = jnp.where(no_prev, BLOCK, 0)
        high = jnp.where(no_next, 2 * BLOCK, 3 * BLOCK)
        shut = jnp.where(jnp.logical_and(spot >= low, spot < high), 0.0, -1e30)
        for part in range(GROUP // HALF):
            lines = slice(part * HALF * BLOCK, (part + 1) * HALF * BLOCK)
            scores = lax.dot_general(
                queries(i, h, part), keys, NT, preferred_element_type=jnp.float32
            )
            scores = scores * SCALE + shut
            top = jnp.max(scores, axis=1, keepdims=True)
            weights = jnp.exp(scores - top)
            summed = jnp.sum(weights, axis=1, keepdims=True)
            acc[n, lines] = jnp.dot(
                weights.astype(jnp.bfloat16), values, preferred_element_type=jnp.float32
            )
            old = stat[lines]
            old = jnp.where(lane == 2 * n, top, old)
            stat[lines] = jnp.where(lane == 2 * n + 1, summed, old)
        return carry

    def far(n, carry):
        i, t, h = place(n)
        gk = jnp.concatenate(
            [gall[t, :, g, 0].reshape(BLOCK, DIM) for g in range(GLOBALS)], axis=0
        )
        gv = jnp.concatenate(
            [gall[t, :, g, 1].reshape(BLOCK, DIM) for g in range(GLOBALS)], axis=0
        )
        entries = pl.ds(i * RANDOM, RANDOM)
        parts = []
        for v in VALUES:
            first, size = CHUNKS[v][1:]
            source, offset = (given[0], first) if first < 64 else (given[1], first - 64)
            parts.append(
                source[t, entries, offset : offset + size, :].reshape(RANDOM * size, DIM)
            )
        for part in range(GROUP // HALF):
            lines = slice(part * HALF * BLOCK, (part + 1) * HALF * BLOCK)
            rows = queries(i, h, part)
            score = lambda keys: SCALE * lax.dot_general(
                rows, keys, NT, preferred_element_type=jnp.float32
            )
            shared = score(gk)
            scores = [score(keys) for keys in parts]
            old = stat[lines]
            top = jnp.sum(jnp.where(lane == 2 * n, old, 0.0), axis=1, keepdims=True)
            summed = jnp.sum(jnp.where(lane == 2 * n + 1, old, 0.0), axis=1, keepdims=True)
            peak = jnp.maximum(top, jnp.max(shared, axis=1, keepdims=True))
            for s in scores:
                peak = jnp.maximum(peak, jnp.max(s, axis=1, keepdims=True))
            shrink = jnp.exp(top - peak)
            weights = jnp.exp(shared - peak)
            summed = summed * shrink + jnp.sum(weights, axis=1, keepdims=True)
            acc[n, lines] = acc[n, lines] * shrink + jnp.dot(
                weights.astype(jnp.bfloat16), gv, preferred_element_type=jnp.float32
            )
            for m, s in enumerate(scores):
                weights = jnp.exp(s - peak)
                summed = summed + jnp.sum(weights, axis=1, keepdims=True)
                probs[m][n, lines] = weights.astype(jnp.bfloat16)
            stat[lines] = jnp.where(lane == 2 * n, 1.0 / summed, old)
        return carry

    def mix(m, n):
        i, t, h = place(n)
        j = VALUES[m]
        size = CHUNKS[j][2]
        values = given[j][t, pl.ds(i * RANDOM, RANDOM)].reshape(RANDOM * size, DIM)
        return i, h, jnp.dot(probs[m][n], values, preferred_element_type=jnp.float32)

    def middle(m):
        def step(n, carry):
            acc[n] = acc[n] + mix(m, n)[2]
            return carry

        return step

    def out_tile(i, h):
        rows = pl.ds(pl.multiple_of(i * BLOCK, BLOCK), BLOCK)
        columns = pl.ds(pl.multiple_of(h * GROUP * DIM, GROUP * DIM), GROUP * DIM)
        return pltpu.make_async_copy(qbuf.at[rows, columns], out_hbm.at[rows, columns], outs)

    def last(n, carry):
        i, h, mixed = mix(len(VALUES) - 1, n)
        wide = lax.broadcasted_iota(jnp.int32, (LINES, DIM), 1)
        scale = jnp.sum(jnp.where(wide == 2 * n, stat[...], 0.0), axis=1, keepdims=True)
        mixed = ((acc[n] + mixed) * scale).astype(jnp.bfloat16)
        rows = pl.ds(pl.multiple_of(i * BLOCK, BLOCK), BLOCK)
        for m in range(GROUP):
            columns = pl.ds(pl.multiple_of((h * GROUP + m) * DIM, DIM), DIM)
            qbuf[rows, columns] = mixed[m * BLOCK : (m + 1) * BLOCK]
        out_tile(i, h).start()
        return carry

    def some(fn, low, high):
        lax.fori_loop(low, high, fn, 0)

    a, b = KEYS
    ring_start(a)
    ring_start(b)
    keep_q.wait()
    keep_k.wait()
    keep_v.wait()
    for side in sides:
        side.wait_recv()
    some(near, 0, 3)
    ring_step(a, 1)
    some(near, 3, 6)
    for j in VALUES:
        own_part(j).wait()
        for t in range(1, XS):
            to_head(j, t).wait_recv()
    split_globals()
    ring_step(b, 1)
    some(near, 6, 9)
    ring_globals()
    ring_step(a, 2)
    some(near, 9, 12)
    pass_globals(0)
    pass_globals(4)
    ring_step(b, 2)
    some(near, 12, 14)
    pass_globals(1)
    pass_globals(5)
    ring_step(a, 3)
    some(near, 14, 16)
    pass_globals(2)
    pass_globals(6)
    ring_step(b, 3)
    pass_globals(3)
    join_globals()
    for j in VALUES:
        hop(j, 0, 1).start()
        hop(j, 1, 1).start()
    ring_step(a, 4)
    spread_globals()
    ring_step(b, 4)
    for j in VALUES:
        choose(j, 0)
    hand_out(a)
    ring_step(VALUES[0], 1)
    hand_out(b)
    ring_step(VALUES[1], 1)
    ring_step(VALUES[2], 1)
    ring_step(VALUES[0], 2)
    for t in range(1, XS):
        widen(t).wait_recv()
    take(a)
    take(b)
    ring_step(VALUES[1], 2)
    some(far, 0, 2)
    ring_step(VALUES[2], 2)
    some(far, 2, 5)
    ring_step(VALUES[0], 3)
    some(far, 5, 8)
    ring_step(VALUES[1], 3)
    some(far, 8, 10)
    ring_step(VALUES[2], 3)
    some(far, 10, 12)
    ring_step(VALUES[0], 4)
    some(far, 12, 14)
    hand_out(VALUES[0])
    ring_step(VALUES[1], 4)
    some(far, 14, 16)
    hand_out(VALUES[1])
    ring_step(VALUES[2], 4)
    take(VALUES[0])
    some(middle(0), 0, 8)
    hand_out(VALUES[2])
    some(middle(0), 8, 16)
    take(VALUES[1])
    some(middle(1), 0, 16)
    take(VALUES[2])
    some(last, 0, 16)

    for j in range(COUNT):
        for t in range(1, XS):
            to_head(j, t).wait_send()
            give(j, t).wait_send()
        for step in range(1, ZS // 2 + 1):
            hop(j, 0, step).wait_send()
            hop(j, 1, step).wait_send()
        pltpu.make_async_copy(outbox[j], outbox[j], ys.at[j]).wait()
    for side in sides:
        side.wait_send()
    whole = gfrom.at[1:PLANE]
    pltpu.make_async_copy(whole, whole, gbs).wait()
    pltpu.make_async_copy(whole, whole, gds).wait()
    for n in range(ZS - 1):
        hop_globals(n).wait_send()
    for t in range(1, XS):
        widen(t).wait_send()
    pltpu.make_async_copy(qbuf, out_hbm, outs).wait()


def on_device(query_rows, key_rows, value_rows, random_table, global_blocks):
    rows, width = query_rows.shape
    seq_count = lax.axis_size("seq")
    seq = lax.axis_index("seq")
    x = lax.axis_index("head")
    z, yc = seq // PLANE, seq % PLANE
    y, c = yc // CS, yc % CS

    refs = lax.dynamic_index_in_dim(random_table, x, 1, keepdims=False)
    refs = refs.reshape(seq_count, RUN * RANDOM)
    plane = lax.dynamic_slice_in_dim(refs, z * PLANE, PLANE, 0)
    up = jnp.arange(ZS, dtype=jnp.int32)
    senders = ((z - up) % ZS) * PLANE + yc
    wanted = jnp.max(
        jnp.where(plane[None] // RUN == senders[:, None, None], plane[None] % RUN, 0), axis=2
    )
    spots = jnp.array([SPOT[d] for d in range(ZS)], jnp.int32)

    def across(owner):
        other = owner % PLANE
        return ((y - other // CS) % YS) * CS + (c - other % CS) % CS

    mine = lax.dynamic_index_in_dim(plane, yc, 0, keepdims=False) // RUN
    up_of = lambda owner: (z - owner // PLANE) % ZS
    lies = across(mine) * ZS + jnp.sum(
        jnp.where(up_of(mine)[:, None] == up[None], spots[None], 0), axis=1
    )
    owners = global_blocks // RUN
    table = jnp.concatenate(
        [wanted.reshape(-1), lies, global_blocks % RUN, across(owners), up_of(owners)]
    )

    vmem = lambda *shape: pltpu.VMEM(shape, jnp.bfloat16)
    dma = pltpu.SemaphoreType.DMA
    sizes = [size for _, _, size in CHUNKS]
    scratch = [
        [[vmem(RUN, r, DIM) for _ in range(ZS)] for r in sizes],
        [vmem(PLANE - 1, ZS, r, DIM) for r in sizes],
        [vmem(PLANE * ZS, r, DIM) for r in sizes],
        [vmem(XS - 1, NAMED, r, DIM) for r in sizes],
        [vmem(XS, NAMED, r, DIM) for r in sizes],
        [vmem(TASKS, LINES, RANDOM * sizes[v]) for v in VALUES],
        vmem(rows, width),
        vmem(HERE + 2, BLOCK, XS * DIM),
        vmem(HERE + 2, BLOCK, XS * DIM),
        pltpu.VMEM((TASKS, LINES, DIM), jnp.float32),
        pltpu.VMEM((LINES, DIM), jnp.float32),
        vmem(PLANE, GLOBALS, 2, PIECE, DIM),
        vmem(PLANE, GLOBALS, 2, PIECE, DIM),
        vmem(ZS, GLOBALS, 2, PIECE, DIM),
        vmem(GLOBALS, 2, PIECE, DIM),
        vmem(XS, PLANE, GLOBALS, 2, PIECE, DIM),
        dma((COUNT, XS - 1)), dma((COUNT, XS - 1)),
        dma((COUNT, 2, ZS // 2)), dma((COUNT, 2, ZS // 2)),
        dma((COUNT,)), dma((COUNT,)),
        dma((COUNT, XS - 1)), dma((COUNT, XS - 1)),
        dma((4,)), dma((4,)),
        dma, dma, dma((ZS - 1,)), dma((ZS - 1,)), dma, dma, dma((XS - 1,)), dma((XS - 1,)),
        dma((COUNT + 3,)), dma,
    ]
    anywhere = pl.BlockSpec(memory_space=pl.ANY)
    blocks = lambda part: part.reshape(HERE, BLOCK, part.shape[1])
    return pl.pallas_call(
        body,
        out_shape=jax.ShapeDtypeStruct((rows, width), jnp.bfloat16),
        in_specs=[pl.BlockSpec(memory_space=pltpu.SMEM)] + [anywhere] * 3,
        out_specs=anywhere,
        scratch_shapes=scratch,
        compiler_params=pltpu.CompilerParams(
            collective_id=0, has_side_effects=True, vmem_limit_bytes=67_043_328
        ),
        name="attend",
    )(table, query_rows, blocks(key_rows), blocks(value_rows))


def solution(mesh):
    split = P(("seq", "head"), None)
    return jax.shard_map(
        on_device,
        mesh=mesh,
        in_specs=(split, split, split, P(), P()),
        out_specs=split,
        check_vma=False,
    )
```

```python
import math

import jax
import jax.numpy as jnp
from jax import lax
from jax.experimental import pallas as pl
from jax.experimental.pallas import tpu as pltpu
from jax.sharding import PartitionSpec as P

BLOCK = 128
DIM = 128
GLOBALS = 2
RANDOM = 3
GROUP = 8
HALF = 4
SCALE = 1.0 / math.sqrt(DIM)
NT = (((1,), (1,)), ((), ()))
MESH = pl.DeviceIdType.MESH

ZS, YS, CS, XS = 8, 4, 2, 4
PLANE = YS * CS
HERE = 4
RUN = HERE * XS
NAMED = HERE * RANDOM
TASKS = HERE * XS
LINES = GROUP * BLOCK
PIECE = BLOCK // PLANE

SIZE = 32
CHUNKS = tuple((kind, first) for kind in (0, 1) for first in range(0, BLOCK, SIZE))
COUNT = len(CHUNKS)
KEYS = range(COUNT // 2)
VALUES = ((4, 5), (6,), (7,))
REACH = 2
SPAN = 2 * REACH + 1
DEPTH = 12
SLOTS = PLANE + PLANE // 2
SPOT = {0: 0, 1: 1, 7: 2, 2: 3, 6: 4, 3: 5, 5: 6, 4: 7}


def body(
    wanted, lies, shared_at, q_hbm, k_hbm, v_hbm, out_hbm,
    ring, relay, slots, middle_slots, outbox, inbox, named, given, probs, qbuf, kwin, vwin, acc, stat,
    gpart, gfrom, gring, gmine, gall,
    x1s, x1r, zs, zr, ys, yr, x2s, x2r, hs, hr,
    gbs, gbr, gcs, gcr, gds, gdr, ghs, ghr, local, outs,
):
    seq = lax.axis_index("seq")
    x = lax.axis_index("head")
    z, yc = seq // PLANE, seq % PLANE
    y, c = yc // CS, yc % CS
    linear = seq * XS + x
    total = ZS * PLANE * XS

    def in_plane(p):
        return lax.rem(y + p // CS, YS) * CS + lax.rem(c + p % CS, CS)

    def at_x(t):
        return lax.rem(x + t, XS)

    above = lax.rem(z + 1, ZS) * PLANE + yc
    below = lax.rem(z + ZS - 1, ZS) * PLANE + yc
    ahead = lax.rem(linear + 1, total)
    behind = lax.rem(linear + total - 1, total)
    ahead = (ahead // XS, lax.rem(ahead, XS))
    behind = (behind // XS, lax.rem(behind, XS))

    def remote(src, dst, send, recv, where):
        return pltpu.make_async_remote_copy(
            src_ref=src, dst_ref=dst, send_sem=send, recv_sem=recv,
            device_id=where, device_id_type=MESH,
        )

    def own_part(j):
        kind, first = CHUNKS[j]
        source = (k_hbm, v_hbm)[kind]
        columns = pl.ds(pl.multiple_of(x * DIM, DIM), DIM)
        return pltpu.make_async_copy(
            source.at[:, first : first + SIZE, columns],
            ring[j][0].at[pl.ds(x * HERE, HERE)],
            local.at[j],
        )

    keep_k = pltpu.make_async_copy(k_hbm, kwin.at[1 : 1 + HERE], local.at[COUNT])
    keep_v = pltpu.make_async_copy(v_hbm, vwin.at[1 : 1 + HERE], local.at[COUNT + 1])
    keep_q = pltpu.make_async_copy(q_hbm, qbuf, local.at[COUNT + 2])

    barrier = pltpu.get_barrier_semaphore()
    partners = [(seq, at_x(t)) for t in range(1, XS)]
    partners += [(z * PLANE + in_plane(p), x) for p in range(1, PLANE)]
    partners += [(lax.rem(z + n, ZS) * PLANE + yc, x) for n in range(1, ZS)]
    partners += [ahead, behind]
    for partner in partners:
        pl.semaphore_signal(barrier, inc=1, device_id=partner, device_id_type=MESH)
    for j in range(COUNT):
        own_part(j).start()
    keep_k.start()
    keep_v.start()
    keep_q.start()
    pl.semaphore_wait(barrier, len(partners))

    def to_head(j, t):
        kind, first = CHUNKS[j]
        source = (k_hbm, v_hbm)[kind]
        columns = pl.ds(pl.multiple_of(at_x(t) * DIM, DIM), DIM)
        return remote(
            source.at[:, first : first + SIZE, columns],
            ring[j][0].at[pl.ds(x * HERE, HERE)],
            x1s.at[j, t - 1], x1r.at[j, t - 1], (seq, at_x(t)),
        )

    for j in range(COUNT):
        for t in range(1, XS):
            to_head(j, t).start()
    sides = [
        remote(k_hbm.at[HERE - 1], kwin.at[0], hs.at[0], hr.at[0], ahead),
        remote(v_hbm.at[HERE - 1], vwin.at[0], hs.at[1], hr.at[1], ahead),
        remote(k_hbm.at[0], kwin.at[HERE + 1], hs.at[2], hr.at[2], behind),
        remote(v_hbm.at[0], vwin.at[HERE + 1], hs.at[3], hr.at[3], behind),
    ]
    for side in sides:
        side.start()

    def hop(j, way, step):
        if step <= REACH:
            before, after = step - 1, step
            if way:
                before, after = (ZS - before) % ZS, ZS - after
            src, dst = ring[j][before], ring[j][after]
        elif step == REACH + 1:
            src, dst = relay[j].at[way], slots[j].at[way]
        else:
            half = PLANE // 2
            src = slots[j].at[way, PLANE:SLOTS]
            dst = middle_slots[j].at[way * half : (way + 1) * half]
        return remote(
            src, dst, zs.at[j, way, step - 1], zr.at[j, way, step - 1],
            (below if way else above, x),
        )

    def named_by(target, origin, place_in_plane):
        return wanted[((target + REACH) * SPAN + origin + REACH) * PLANE + place_in_plane]

    def prepare(j, way):
        sign = -1 if way else 1
        source = ring[j][ZS - REACH if way else REACH]
        for r in range(PLANE):
            relay[j][way, r] = source[named_by(sign, -REACH * sign, r)]
        for r in range(PLANE // 2):
            further = r + (PLANE // 2 if way else 0)
            relay[j][way, PLANE + r] = source[named_by(2 * sign, -REACH * sign, further)]

    def choose(j, d):
        for p in range(PLANE):
            there = in_plane(p)
            if d <= REACH:
                block = ring[j][d][named_by(0, -d, there)]
            elif d >= ZS - REACH:
                block = ring[j][d][named_by(0, ZS - d, there)]
            elif d == ZS // 2:
                block = middle_slots[j][there]
            else:
                block = slots[j][0 if d < ZS // 2 else 1, there]
            if p:
                outbox[j][p - 1, SPOT[d]] = block
            else:
                inbox[j][SPOT[d]] = block

    def post(j, low, high):
        for p in range(1, PLANE):
            remote(
                outbox[j].at[p - 1, low:high],
                inbox[j].at[p * ZS + low : p * ZS + high],
                ys.at[j], yr.at[j], (z * PLANE + in_plane(p), x),
            ).start()

    ready = set()

    def ring_ready(j):
        if j in ready:
            return
        ready.add(j)
        own_part(j).wait()
        for t in range(1, XS):
            to_head(j, t).wait_recv()

    def ring_start(j):
        hop(j, 0, 1).start()
        hop(j, 1, 1).start()
        choose(j, 0)

    def ring_step(j, step):
        hop(j, 0, step).wait_recv()
        hop(j, 1, step).wait_recv()
        if step == REACH:
            prepare(j, 0)
            prepare(j, 1)
        if step < ZS // 2:
            hop(j, 0, step + 1).start()
            hop(j, 1, step + 1).start()
            choose(j, step)
            choose(j, ZS - step)
            low = 0 if step == 1 else 2 * step - 1
            post(j, low, 2 * step + 1)
        else:
            choose(j, step)
            post(j, ZS - 1, ZS)

    def give(j, t):
        return remote(
            named[j].at[t - 1], given[j].at[t], x2s.at[j, t - 1], x2r.at[j, t - 1],
            (seq, at_x(t)),
        )

    def hand_out(j):
        whole = inbox[j].at[ZS : PLANE * ZS]
        pltpu.make_async_copy(whole, whole, yr.at[j]).wait()
        for t in [1, 2, 3, 0]:
            base = at_x(t) * NAMED

            def entry(e, carry):
                block = inbox[j][lies[base + e]]
                if t:
                    named[j][t - 1, e] = block
                else:
                    given[j][0, e] = block
                return carry

            lax.fori_loop(0, NAMED, entry, 0)
            if t:
                give(j, t).start()

    def take(j):
        for t in range(1, XS):
            give(j, t).wait_recv()

    def split_globals():
        for g in range(GLOBALS):
            block = shared_at[g]
            for j in range(COUNT):
                kind, first = CHUNKS[j]
                rows = ring[j][0][block]
                for a in range(SIZE // PIECE):
                    gpart[first // PIECE + a, g, kind] = rows[a * PIECE : (a + 1) * PIECE]
        gfrom[0] = gpart[yc]
        for p in range(1, PLANE):
            there = in_plane(p)
            remote(
                gpart.at[there], gfrom.at[p], gbs, gbr, (z * PLANE + there, x)
            ).start()

    def to_plane(n):
        there = lax.rem(z + n, ZS) * PLANE + yc
        return remote(gring.at[0], gring.at[n], gcs.at[n - 1], gcr.at[n - 1], (there, x))

    def ring_globals():
        whole = gfrom.at[1:PLANE]
        pltpu.make_async_copy(whole, whole, gbr).wait()
        for g in range(GLOBALS):
            gring[0, g] = gfrom[shared_at[GLOBALS + g], g]
        for n in range(1, ZS):
            to_plane(n).start()

    def join_globals():
        for n in range(1, ZS):
            to_plane(n).wait_recv()
        for g in range(GLOBALS):
            piece = gring[shared_at[2 * GLOBALS + g], g]
            gmine[g] = piece
            gall[0, yc, g] = piece
        for p in range(1, PLANE):
            remote(
                gmine, gall.at[0, yc], gds, gdr, (z * PLANE + in_plane(p), x)
            ).start()

    def widen(t):
        return remote(gall.at[0], gall.at[t], ghs.at[t - 1], ghr.at[t - 1], (seq, at_x(t)))

    def spread_globals():
        whole = gfrom.at[1:PLANE]
        pltpu.make_async_copy(whole, whole, gdr).wait()
        for t in range(1, XS):
            widen(t).start()

    lane = lax.broadcasted_iota(jnp.int32, (HALF * BLOCK, DIM), 1)

    def place(n):
        i, t = n // XS, lax.rem(n, XS)
        return i, t, lax.rem(x + XS - t, XS)

    def queries(i, h, part):
        first = (h * GROUP + part * HALF) * DIM
        rows = pl.ds(pl.multiple_of(i * BLOCK, BLOCK), BLOCK)
        return jnp.concatenate(
            [
                qbuf[rows, pl.ds(pl.multiple_of(first + m * DIM, DIM), DIM)]
                for m in range(HALF)
            ],
            axis=0,
        )

    def near(n, carry):
        i, t, h = place(n)
        columns = pl.ds(pl.multiple_of(h * DIM, DIM), DIM)
        keys = kwin[pl.ds(i, 3), :, columns].reshape(3 * BLOCK, DIM)
        values = vwin[pl.ds(i, 3), :, columns].reshape(3 * BLOCK, DIM)
        no_prev = jnp.logical_and(linear == 0, i == 0)
        no_next = jnp.logical_and(linear == total - 1, i == HERE - 1)
        spot = lax.broadcasted_iota(jnp.int32, (1, 3 * BLOCK), 1)
        low = jnp.where(no_prev, BLOCK, 0)
        high = jnp.where(no_next, 2 * BLOCK, 3 * BLOCK)
        shut = jnp.where(jnp.logical_and(spot >= low, spot < high), 0.0, -1e30)
        for part in range(GROUP // HALF):
            lines = slice(part * HALF * BLOCK, (part + 1) * HALF * BLOCK)
            scores = lax.dot_general(
                queries(i, h, part), keys, NT, preferred_element_type=jnp.float32
            )
            scores = scores * SCALE + shut
            top = jnp.max(scores, axis=1, keepdims=True)
            weights = jnp.exp(scores - top)
            summed = jnp.sum(weights, axis=1, keepdims=True)
            acc[n, lines] = jnp.dot(
                weights.astype(jnp.bfloat16), values, preferred_element_type=jnp.float32
            )
            old = stat[lines]
            old = jnp.where(lane == 2 * n, top, old)
            stat[lines] = jnp.where(lane == 2 * n + 1, summed, old)
        return carry

    def far(n, carry):
        i, t, h = place(n)
        gk = jnp.concatenate(
            [gall[t, :, g, 0].reshape(BLOCK, DIM) for g in range(GLOBALS)], axis=0
        )
        gv = jnp.concatenate(
            [gall[t, :, g, 1].reshape(BLOCK, DIM) for g in range(GLOBALS)], axis=0
        )
        entries = pl.ds(i * RANDOM, RANDOM)
        keys = jnp.concatenate(
            [gk] + [given[j][t, entries].reshape(RANDOM * SIZE, DIM) for j in KEYS], axis=0
        )
        split = GLOBALS * BLOCK
        for part in range(GROUP // HALF):
            lines = slice(part * HALF * BLOCK, (part + 1) * HALF * BLOCK)
            rows = queries(i, h, part)
            scores = SCALE * lax.dot_general(
                rows, keys, NT, preferred_element_type=jnp.float32
            )
            old = stat[lines]
            top = jnp.sum(jnp.where(lane == 2 * n, old, 0.0), axis=1, keepdims=True)
            summed = jnp.sum(jnp.where(lane == 2 * n + 1, old, 0.0), axis=1, keepdims=True)
            peak = jnp.maximum(top, jnp.max(scores, axis=1, keepdims=True))
            shrink = jnp.exp(top - peak)
            weights = jnp.exp(scores - peak)
            summed = summed * shrink + jnp.sum(weights, axis=1, keepdims=True)
            weights = weights.astype(jnp.bfloat16)
            acc[n, lines] = acc[n, lines] * shrink + jnp.dot(
                weights[:, :split], gv, preferred_element_type=jnp.float32
            )
            probs[n, lines] = weights[:, split:]
            stat[lines] = jnp.where(lane == 2 * n, 1.0 / summed, old)
        return carry

    def mix(m, n):
        i, t, h = place(n)
        rows = RANDOM * SIZE
        first = (VALUES[m][0] - COUNT // 2) * rows
        end = first + len(VALUES[m]) * rows
        low, high = first // DIM * DIM, -(-end // DIM) * DIM
        entries = pl.ds(i * RANDOM, RANDOM)
        values = [given[j][t, entries].reshape(rows, DIM) for j in VALUES[m]]
        if first > low:
            values = [jnp.zeros((first - low, DIM), jnp.bfloat16)] + values
        if high > end:
            values = values + [jnp.zeros((high - end, DIM), jnp.bfloat16)]
        mixed = jnp.dot(
            probs[n, :, low:high], jnp.concatenate(values, axis=0),
            preferred_element_type=jnp.float32,
        )
        return i, h, mixed

    def middle(m):
        def step(n, carry):
            acc[n] = acc[n] + mix(m, n)[2]
            return carry

        return step

    def out_tile(i, h):
        rows = pl.ds(pl.multiple_of(i * BLOCK, BLOCK), BLOCK)
        columns = pl.ds(pl.multiple_of(h * GROUP * DIM, GROUP * DIM), GROUP * DIM)
        return pltpu.make_async_copy(qbuf.at[rows, columns], out_hbm.at[rows, columns], outs)

    def last(n, carry):
        i, h, mixed = mix(len(VALUES) - 1, n)
        wide = lax.broadcasted_iota(jnp.int32, (LINES, DIM), 1)
        scale = jnp.sum(jnp.where(wide == 2 * n, stat[...], 0.0), axis=1, keepdims=True)
        mixed = ((acc[n] + mixed) * scale).astype(jnp.bfloat16)
        rows = pl.ds(pl.multiple_of(i * BLOCK, BLOCK), BLOCK)
        for m in range(GROUP):
            columns = pl.ds(pl.multiple_of((h * GROUP + m) * DIM, DIM), DIM)
            qbuf[rows, columns] = mixed[m * BLOCK : (m + 1) * BLOCK]
        out_tile(i, h).start()
        return carry

    cost = {1: 4, 2: 4, 3: 3, 4: 1}
    queue, begun, ahead_of = [], 0, 0
    after = {}

    def at(event, *parts):
        after.setdefault(event, []).extend(parts)

    def tasks(fn, low, high):
        return lambda: lax.fori_loop(low, high, fn, 0)

    def call(fn, *args):
        return lambda: fn(*args)

    def windows():
        keep_q.wait()
        keep_k.wait()
        keep_v.wait()
        for side in sides:
            side.wait_recv()

    def globals_ready():
        for j in range(COUNT):
            ring_ready(j)
        split_globals()

    def far_ready():
        for t in range(1, XS):
            widen(t).wait_recv()
        for j in KEYS:
            take(j)

    at(1, windows, tasks(near, 0, 2))
    at(3, tasks(near, 2, 5))
    at(5, tasks(near, 5, 8))
    at(6, globals_ready)
    at(8, tasks(near, 8, 12))
    at(9, ring_globals)
    at(11, tasks(near, 12, 16))
    at(13, join_globals)
    at(15, spread_globals)
    FAR = 25
    at(FAR, far_ready, tasks(far, 0, 2))
    at(FAR + 2, tasks(far, 2, 5))
    at(FAR + 4, tasks(far, 5, 8))
    at(FAR + 5, tasks(far, 8, 9))

    def begin():
        nonlocal begun, ahead_of
        while begun < COUNT and ahead_of < DEPTH:
            ring_ready(begun)
            ring_start(begun)
            queue.append((begun, 1))
            ahead_of += cost[1]
            begun += 1

    begin()
    event = 0
    handed = []
    while queue:
        j, step = queue.pop(0)
        ring_step(j, step)
        ahead_of -= cost[step]
        if step < ZS // 2:
            queue.append((j, step + 1))
            ahead_of += cost[step + 1]
        elif event + 2 < COUNT * ZS // 2 - 1:
            at(event + 2, call(hand_out, j))
            handed.append(j)
        begin()
        for part in after.pop(event, ()):
            part()
        event += 1
    rest = [j for j in range(COUNT) if j not in handed]
    lax.fori_loop(9, 11, far, 0)
    for j in rest:
        hand_out(j)
    lax.fori_loop(11, TASKS, far, 0)
    take(4)
    take(5)
    lax.fori_loop(0, TASKS, middle(0), 0)
    take(6)
    lax.fori_loop(0, TASKS, middle(1), 0)
    take(7)
    lax.fori_loop(0, TASKS, last, 0)

    for j in range(COUNT):
        for t in range(1, XS):
            to_head(j, t).wait_send()
            give(j, t).wait_send()
        for step in range(1, ZS // 2 + 1):
            hop(j, 0, step).wait_send()
            hop(j, 1, step).wait_send()
        pltpu.make_async_copy(outbox[j], outbox[j], ys.at[j]).wait()
    for side in sides:
        side.wait_send()
    whole = gfrom.at[1:PLANE]
    pltpu.make_async_copy(whole, whole, gbs).wait()
    pltpu.make_async_copy(whole, whole, gds).wait()
    for n in range(1, ZS):
        to_plane(n).wait_send()
    for t in range(1, XS):
        widen(t).wait_send()
    pltpu.make_async_copy(qbuf, out_hbm, outs).wait()


def on_device(query_rows, key_rows, value_rows, random_table, global_blocks):
    rows, width = query_rows.shape
    seq_count = lax.axis_size("seq")
    seq = lax.axis_index("seq")
    x = lax.axis_index("head")
    z, yc = seq // PLANE, seq % PLANE
    y, c = yc // CS, yc % CS

    refs = lax.dynamic_index_in_dim(random_table, x, 1, keepdims=False)
    refs = refs.reshape(ZS, PLANE, RUN * RANDOM)
    near_by = lax.dynamic_slice_in_dim(
        jnp.concatenate([refs, refs], axis=0), (z + ZS - REACH) % ZS, SPAN, 0
    )
    origins = ((z + jnp.arange(-REACH, REACH + 1, dtype=jnp.int32)) % ZS) * PLANE + yc
    named_runs = near_by[:, None] // RUN == origins[None, :, None, None]
    wanted = jnp.max(jnp.where(named_runs, near_by[:, None] % RUN, 0), axis=3)

    def across(owner):
        other = owner % PLANE
        return ((y - other // CS) % YS) * CS + (c - other % CS) % CS

    mine = lax.dynamic_index_in_dim(near_by[REACH], yc, 0, keepdims=False) // RUN
    up_of = lambda owner: (z - owner // PLANE) % ZS
    spot = jnp.zeros_like(mine)
    for d in range(ZS):
        spot = jnp.where(up_of(mine) == d, SPOT[d], spot)
    lies = across(mine) * ZS + spot
    owners = global_blocks // RUN
    shared_at = jnp.concatenate([global_blocks % RUN, across(owners), up_of(owners)])

    vmem = lambda *shape: pltpu.VMEM(shape, jnp.bfloat16)
    dma = pltpu.SemaphoreType.DMA
    every = lambda *shape: [vmem(*shape) for _ in range(COUNT)]
    passed = [d for d in range(ZS) if d <= REACH or d >= ZS - REACH]
    scratch = [
        [{d: vmem(RUN, SIZE, DIM) for d in passed} for _ in range(COUNT)],
        every(2, SLOTS, SIZE, DIM),
        every(2, SLOTS, SIZE, DIM),
        every(PLANE, SIZE, DIM),
        every(PLANE - 1, ZS, SIZE, DIM),
        every(PLANE * ZS, SIZE, DIM),
        every(XS - 1, NAMED, SIZE, DIM),
        every(XS, NAMED, SIZE, DIM),
        vmem(TASKS, LINES, RANDOM * BLOCK),
        vmem(rows, width),
        vmem(HERE + 2, BLOCK, XS * DIM),
        vmem(HERE + 2, BLOCK, XS * DIM),
        pltpu.VMEM((TASKS, LINES, DIM), jnp.float32),
        pltpu.VMEM((LINES, DIM), jnp.float32),
        vmem(PLANE, GLOBALS, 2, PIECE, DIM),
        vmem(PLANE, GLOBALS, 2, PIECE, DIM),
        vmem(ZS, GLOBALS, 2, PIECE, DIM),
        vmem(GLOBALS, 2, PIECE, DIM),
        vmem(XS, PLANE, GLOBALS, 2, PIECE, DIM),
        dma((COUNT, XS - 1)), dma((COUNT, XS - 1)),
        dma((COUNT, 2, ZS // 2)), dma((COUNT, 2, ZS // 2)),
        dma((COUNT,)), dma((COUNT,)),
        dma((COUNT, XS - 1)), dma((COUNT, XS - 1)),
        dma((4,)), dma((4,)),
        dma, dma, dma((ZS - 1,)), dma((ZS - 1,)), dma, dma, dma((XS - 1,)), dma((XS - 1,)),
        dma((COUNT + 3,)), dma,
    ]
    anywhere = pl.BlockSpec(memory_space=pl.ANY)
    blocks = lambda part: part.reshape(HERE, BLOCK, part.shape[1])
    return pl.pallas_call(
        body,
        out_shape=jax.ShapeDtypeStruct((rows, width), jnp.bfloat16),
        in_specs=[pl.BlockSpec(memory_space=pltpu.SMEM)] * 3 + [anywhere] * 3,
        out_specs=anywhere,
        scratch_shapes=scratch,
        compiler_params=pltpu.CompilerParams(
            collective_id=0, has_side_effects=True, vmem_limit_bytes=67_043_328
        ),
        name="attend",
    )(wanted.reshape(-1), lies, shared_at, query_rows, blocks(key_rows), blocks(value_rows))


def solution(mesh):
    split = P(("seq", "head"), None)
    return jax.shard_map(
        on_device,
        mesh=mesh,
        in_specs=(split, split, split, P(), P()),
        out_specs=split,
        check_vma=False,
    )
```
